32 devices in a mesh: job: 2 (over y), ta: 4 (over z), xyz: 2 (over x), src: 2 (over core).
Axes of the slice: x: 2, y: 2, z: 4, core: 2. Of those that a mesh axis runs over, the one named last changes fastest.
Arguments:
- spinors: float32 [64, 8, 2, 8, 3, 512], P('src', 'ta', None, 'job', None, 'xyz'), parts along dimension 3, may hold values from -6 to 6
- eigvecs: float32 [8, 256, 2, 3, 512], P('ta', 'job', None, None, 'xyz'), parts along dimension 1, may hold values from -0.109375 to 0.109375
- group_of: int32 [8], replicated, may hold values from 0 to 3, as said below
- source_ids: int32 [64], P('src'), may hold values from 0 to 63, as said below
Outputs:
- perambulator: float32 [8, 2, 8, 64, 128], P('ta', None, 'job', 'src', 'xyz'), parts along dimension 2
The draws below stay inside these ranges and needn't reach their ends.
There are 2 independent parts, one for each index of `job`. The reference program is written for one: setup_inputs(seed, part) draws one part's arguments, and reference() takes and returns one part's arrays. A program takes and returns all parts, laid end to end along the dimension named above; an argument that names none is the same for every part. Nothing has to cross between parts.
Inputs may be any that keep to these rules, and one draw needn't show every extreme that they name: `group_of`: every group number appears exactly 2 times. `source_ids`: the 32 entries held by index i of src are a permutation of i * 32 to (i + 1) * 32 - 1.
All inputs are finite; a program needn't handle non-finite values.
Results may differ from the reference program's by a relative error of at most 0.00007.
Values sent between devices are 32-bit elements; how exact they have to be, the bound alone decides.
A program may use at most 64 MiB of HBM per device.

```python
import jax
import jax.numpy as jnp
from jax import lax

K = 128
TL = 2
NS = 32
NT = 8
SITES = 512
NSRC = 64


def draw_group_of(key, part):
    scores = jax.random.randint(key, (NT,), 0, 1 << 20) * NT + jnp.arange(NT, dtype=jnp.int32)
    shuffle = jnp.argsort(scores).astype(jnp.int32)
    return (jnp.argsort(shuffle).astype(jnp.int32) // TL).astype(jnp.int32)


def draw_source_ids(key, part):
    scores = jax.random.randint(key, (NSRC,), 0, 1 << 20) * NSRC + jnp.arange(NSRC, dtype=jnp.int32)
    blocks = scores.reshape(NSRC // NS, NS)
    within = jnp.argsort(blocks, axis=1).astype(jnp.int32)
    offsets = (jnp.arange(NSRC // NS, dtype=jnp.int32) * NS)[:, None]
    return (within + offsets).reshape(NSRC).astype(jnp.int32)


def levels(own_key, shape, pieces, least, top_value):
    def one(dim, blocks):
        steps = jax.random.uniform(jax.random.fold_in(jax.random.fold_in(own_key, 6), dim), (blocks,), jnp.float32, least / len(pieces), top_value / len(pieces))
        return jnp.repeat(jnp.exp(steps), shape[dim] // blocks).reshape((-1,) + (1,) * (len(shape) - dim - 1))

    loudness = one(*pieces[0])
    for cut in pieces[1:]:
        loudness = loudness * one(*cut)
    return loudness


def centred(rng, shape, width, most, cuts=(), kind=jnp.bfloat16):
    entries = width * jax.random.normal(rng, shape, jnp.float32)
    if cuts:
        entries = entries * levels(rng, shape, cuts, -0.22, 0.18)
    return jnp.clip(entries, -most, most).astype(kind)


def setup_inputs(seed: int = 0, part: int = 0) -> dict:
    streams_of = jax.random.split(jax.random.key(seed), 5)
    part_splits = jax.random.split(jax.random.fold_in(streams_of[4], part), 5)
    return {
        "spinors": centred(part_splits[0], (NSRC, NT, 2, 4, 3, SITES), 1.0, 6.0, ((0, 2), (1, 4), (5, 2)), jnp.float32),
        "eigvecs": centred(part_splits[1], (NT, K, 2, 3, SITES), (6 * SITES) ** -0.5, 0.109375, ((0, 4), (4, 2)), jnp.float32),
        "group_of": draw_group_of(jax.random.fold_in(streams_of[4], 71), part),
        "source_ids": draw_source_ids(jax.random.fold_in(streams_of[4], 71), part),
    }


def contract_pair(vectors, spinor):
    vector_real = vectors[:, :, 0]
    vector_imag = vectors[:, :, 1]
    spinor_real = spinor[:, :, 0]
    spinor_imag = spinor[:, :, 1]

    def contract(left_side, right_side):
        return jnp.einsum("tkcx,ntscx->tsnk", left_side, right_side, precision=lax.Precision.HIGHEST)

    real_part = contract(vector_real, spinor_real) + contract(vector_imag, spinor_imag)
    imag_part = contract(vector_real, spinor_imag) - contract(vector_imag, spinor_real)
    return jnp.stack([real_part, imag_part], axis=1)


def reference(spinors, eigvecs, group_of, source_ids):
    extent = group_of.shape[0]
    sort_keys = group_of.astype(jnp.int32) * extent + jnp.arange(extent, dtype=jnp.int32)
    ordering = jnp.argsort(sort_keys).astype(jnp.int32)

    def one_slice(position):
        timeslice = ordering[position]
        vectors = lax.dynamic_slice_in_dim(eigvecs, position, 1, 0)
        spinor = lax.dynamic_slice_in_dim(spinors, timeslice, 1, 1)
        return contract_pair(vectors, spinor)[0]

    projected = lax.map(one_slice, jnp.arange(extent, dtype=jnp.int32))
    inverse = jnp.argsort(source_ids).astype(jnp.int32)
    return jnp.take(projected, inverse, axis=3)
```

```python
import functools

import jax
import jax.numpy as jnp
from jax import lax
from jax.experimental import pallas as pl
from jax.experimental.pallas import tpu as pltpu
from jax.sharding import PartitionSpec as P

MESH = pl.DeviceIdType.MESH
OUT_PIECES = 2


def contract_pair(vectors, spinor):
    vector_real = vectors[:, :, 0]
    vector_imag = vectors[:, :, 1]
    spinor_real = spinor[:, :, 0]
    spinor_imag = spinor[:, :, 1]

    def contract(left_side, right_side):
        return jnp.einsum(
            "tkcx,ntscx->tsnk", left_side, right_side, precision=lax.Precision.HIGHEST
        )

    real_part = contract(vector_real, spinor_real) + contract(vector_imag, spinor_imag)
    imag_part = contract(vector_real, spinor_imag) - contract(vector_imag, spinor_real)
    return jnp.stack([real_part, imag_part], axis=1)


def local_general(spinors, eigvecs, group_of, source_ids):
    extent = group_of.shape[0]
    sort_keys = group_of * extent + jnp.arange(extent, dtype=jnp.int32)
    ordering = jnp.argsort(sort_keys)
    spread = lax.all_to_all(spinors, "ta", split_axis=0, concat_axis=1, tiled=True)
    grouped = jnp.take(spread, ordering, axis=1)
    regrouped = lax.all_to_all(grouped, "ta", split_axis=1, concat_axis=0, tiled=True)
    partial_sums = contract_pair(eigvecs, regrouped)
    summed = lax.psum_scatter(partial_sums, "xyz", scatter_dimension=4, tiled=True)
    inverse = jnp.argsort(source_ids)
    return jnp.take(summed, inverse, axis=3)


def copy_to(src, dst, sems, index, where):
    return pltpu.make_async_remote_copy(
        src_ref=src,
        dst_ref=dst,
        send_sem=sems.at[0, index],
        recv_sem=sems.at[1, index],
        device_id=where,
        device_id_type=MESH,
    )


def kernel(n, m, pieces, tab, e_ref, s_ref, out_ref, *scratch):
    held = e_ref.shape[0]
    scratch = list(scratch)

    def take(count):
        got = scratch[:count]
        del scratch[:count]
        return got

    side_e, mid_e, recv_e, give_e = take(pieces), take(pieces), take(pieces), take(pieces)
    side_o, mid_o, recv_o, give_o = (
        take(OUT_PIECES), take(OUT_PIECES), take(OUT_PIECES), take(OUT_PIECES)
    )
    full, high, low, acc, x_recv, o_recv, o_send = take(7)
    in_e, cross_e, back_e, core_e, x_sem, in_o, cross_o, back_o = take(8)

    z = lax.axis_index("ta")
    core = lax.axis_index("src")
    xi = lax.axis_index("xyz")
    right = z // (n // 2)
    inner = jnp.logical_and(z > 0, z < n - 1)
    outer = jnp.logical_not(inner)
    to_inner = {"ta": 1 + right}
    to_outer = {"ta": right * (n - 1)}
    to_other = {"ta": n - 1 - z}
    to_core = {"src": 1 - core}
    to_x = {"xyz": 1 - xi}
    outer_at = right * held
    own_at = (1 - right) * held
    depth = e_ref.shape[2] // 2
    half_rows = pl.ds(pl.multiple_of(core * depth, depth), depth)
    other_rows = pl.ds(pl.multiple_of((1 - core) * depth, depth), depth)

    barrier = pltpu.get_barrier_semaphore()
    for where in (to_core, to_x):
        pl.semaphore_signal(barrier, inc=1, device_id=where, device_id_type=MESH)

    @pl.when(inner)
    def _():
        for where in (to_outer, to_other):
            pl.semaphore_signal(barrier, inc=1, device_id=where, device_id_type=MESH)
        pl.semaphore_wait(barrier, 4)

    @pl.when(outer)
    def _():
        pl.semaphore_signal(barrier, inc=1, device_id=to_inner, device_id_type=MESH)
        pl.semaphore_wait(barrier, 3)

    def mine(j):
        return e_ref.at[:, j, half_rows, :]

    def inward_e(j):
        return copy_to(mine(j), side_e[j].at[pl.ds(outer_at, held)], in_e, j, to_inner)

    def across_e(j):
        return copy_to(mid_e[j], recv_e[j], cross_e, j, to_other)

    def back_out_e(j):
        return copy_to(give_e[j], full.at[j, :, half_rows, :], back_e, j, to_outer)

    def swap_e(j):
        view = full.at[j, :, half_rows, :]
        return copy_to(view, view, core_e, j, to_core)

    def swapped_e(j):
        view = full.at[j, :, other_rows, :]
        return copy_to(view, view, core_e, j, to_core)

    def chosen(which, q, side, recv):
        own = side[tab[which, 1, q]]
        far = recv[tab[which, 2, q]]
        return jnp.where(tab[which, 3, q] == 1, own, far)

    @pl.when(outer)
    def _():
        for j in range(pieces):
            inward_e(j).start()

    @pl.when(inner)
    def _():
        for j in range(pieces):
            side_e[j][pl.ds(own_at, held)] = e_ref[:, j, half_rows, :]

    def split(value):
        top = value.astype(jnp.bfloat16)
        return top, (value - top.astype(jnp.float32)).astype(jnp.bfloat16)

    colours = s_ref.shape[2]
    width = s_ref.shape[3]

    for t in range(held):
        acc[t] = jnp.zeros(acc.shape[1:], jnp.float32)
        for c in range(colours):
            real_top, real_low = split(s_ref[t, 0, c])
            imag_top, imag_low = split(s_ref[t, 1, c])
            for keep, real, imag in ((high, real_top, imag_top), (low, real_low, imag_low)):
                keep[t, 2 * c, :width] = real
                keep[t, 2 * c, width:] = imag
                keep[t, 2 * c + 1, :width] = imag
                keep[t, 2 * c + 1, width:] = -real

    @pl.when(inner)
    def _():
        def finish(j):
            across_e(j).wait_recv()
            for i in range(held):
                give_e[j][i] = chosen(0, outer_at + i, side_e[j], recv_e[j])
            back_out_e(j).start()
            for i in range(held):
                full[j, i, half_rows, :] = chosen(0, own_at + i, side_e[j], recv_e[j])
            swap_e(j).start()

        for j in range(pieces):
            inward_e(j).wait_recv()
            for slot in range(m):
                mid_e[j][slot] = side_e[j][tab[0, 0, slot]]
            across_e(j).start()
            if j > 0:
                finish(j - 1)
        finish(pieces - 1)
        for j in range(pieces):
            across_e(j).wait_send()
            back_out_e(j).wait_send()

    @pl.when(outer)
    def _():
        for j in range(pieces):
            back_out_e(j).wait_recv()
            swap_e(j).start()
        for j in range(pieces):
            inward_e(j).wait_send()

    for j in range(pieces):
        swapped_e(j).wait_recv()

    def step(j, carry):
        for t in range(held):
            top, rest = split(full[j, t])

            def dot(a, b):
                return lax.dot_general(
                    a, b, (((1,), (1,)), ((), ())), preferred_element_type=jnp.float32
                )

            acc[t] += dot(top, high[t, j]) + (dot(top, low[t, j]) + dot(rest, high[t, j]))
        return carry

    lax.fori_loop(0, pieces, step, 0)
    for j in range(pieces):
        swap_e(j).wait_send()

    rows = acc.shape[1] // 2
    part = rows // OUT_PIECES

    def x_swap(q):
        there = pl.ds(pl.multiple_of((1 - xi) * rows + q * part, part), part)
        return copy_to(acc.at[:, there, :], x_recv.at[q], x_sem, q, to_x)

    def summed(q):
        here = pl.ds(pl.multiple_of(xi * rows + q * part, part), part)
        return acc[:, here, :] + x_recv[q]

    def inward_o(q):
        return copy_to(o_send.at[q], side_o[q].at[pl.ds(outer_at, held)], in_o, q, to_inner)

    def across_o(q):
        return copy_to(mid_o[q], recv_o[q], cross_o, q, to_other)

    def back_out_o(q):
        return copy_to(give_o[q], o_recv.at[q], back_o, q, to_outer)

    for q in range(OUT_PIECES):
        x_swap(q).start()

    @pl.when(outer)
    def _():
        for q in range(OUT_PIECES):
            x_swap(q).wait_recv()
            o_send[q] = summed(q)
            inward_o(q).start()
        for q in range(OUT_PIECES):
            back_out_o(q).wait_recv()
            out_ref[:, q * part:(q + 1) * part, :] = o_recv[q]
        for q in range(OUT_PIECES):
            inward_o(q).wait_send()

    @pl.when(inner)
    def _():
        for q in range(OUT_PIECES):
            x_swap(q).wait_recv()
            side_o[q][pl.ds(own_at, held)] = summed(q)
        for q in range(OUT_PIECES):
            inward_o(q).wait_recv()
            for slot in range(m):
                mid_o[q][slot] = side_o[q][tab[1, 0, slot]]
            across_o(q).start()
        for q in range(OUT_PIECES):
            across_o(q).wait_recv()
            for i in range(held):
                give_o[q][i] = chosen(1, outer_at + i, side_o[q], recv_o[q])
            back_out_o(q).start()
            for i in range(held):
                out_ref[i, q * part:(q + 1) * part, :] = chosen(
                    1, own_at + i, side_o[q], recv_o[q]
                )
        for q in range(OUT_PIECES):
            across_o(q).wait_send()
            back_out_o(q).wait_send()

    for q in range(OUT_PIECES):
        x_swap(q).wait_send()


def local_line(n, spinors, eigvecs, group_of, source_ids):
    extent = group_of.shape[0]
    half = extent // 2
    sources, held, _, spins, colours, sites = spinors.shape
    vectors = eigvecs.shape[1]
    pieces = 2 * colours
    depth = vectors // 2
    width = spins * sources

    items = jnp.arange(extent, dtype=jnp.int32)
    keys = group_of * extent + items
    rank = jnp.sum((keys[None, :] < keys[:, None]).astype(jnp.int32), axis=1)
    match = rank[None, :] == items[:, None]
    ordering = jnp.sum(jnp.where(match, items[None, :], 0), axis=1)
    right = lax.axis_index("ta") // (n // 2)
    spot = jnp.arange(half, dtype=jnp.int32)

    def tables(wanted, goes_to):
        crosses = (goes_to // half) != (items // half)
        same = (items // half)[:, None] == (items // half)[None, :]
        before = crosses[None, :] & same & (items[None, :] < items[:, None])
        slot = jnp.sum(before.astype(jnp.int32), axis=1)
        leaving = crosses & ((items // half) == right)
        send = jnp.sum(
            jnp.where(leaving[None, :] & (slot[None, :] == spot[:, None]), items[None, :] % half, 0),
            axis=1,
        )
        here = items[None, :] == (spot + right * half)[:, None]
        want = jnp.sum(jnp.where(here, wanted[None, :], 0), axis=1)
        own = (want // half) == right
        far = jnp.sum(jnp.where(items[None, :] == want[:, None], slot[None, :], 0), axis=1)
        table = jnp.stack([
            send,
            jnp.where(own, want % half, 0),
            jnp.where(own, 0, far),
            own.astype(jnp.int32),
        ])
        return table, jnp.sum(jnp.where(items < half, crosses.astype(jnp.int32), 0))

    table_e, count = tables(rank, ordering)
    table_o, _ = tables(ordering, rank)
    table = jnp.stack([table_e, table_o])

    e_view = eigvecs.transpose(0, 3, 2, 1, 4).reshape(held, pieces, vectors, sites)
    s_view = spinors.transpose(1, 2, 4, 3, 0, 5).reshape(held, 2, colours, width, sites)

    rows = vectors // 2
    part = rows // OUT_PIECES
    f32 = jnp.float32

    def run(m):
        vmem = pl.BlockSpec(memory_space=pltpu.VMEM)
        e_item = (depth, sites)
        o_item = (part, 2 * width)
        buffers = []
        for count_, item in ((pieces, e_item), (OUT_PIECES, o_item)):
            for slots in (half, m, m, held):
                buffers += [pltpu.VMEM((slots,) + item, f32)] * count_
        return pl.pallas_call(
            functools.partial(kernel, n, m, pieces),
            name=f"project_{m}",
            out_shape=jax.ShapeDtypeStruct((held, rows, 2 * width), f32),
            in_specs=[pl.BlockSpec(memory_space=pltpu.SMEM), vmem, vmem],
            out_specs=vmem,
            scratch_shapes=buffers + [
                pltpu.VMEM((pieces, held, vectors, sites), f32),
                pltpu.VMEM((held, pieces, 2 * width, sites), jnp.bfloat16),
                pltpu.VMEM((held, pieces, 2 * width, sites), jnp.bfloat16),
                pltpu.VMEM((held, vectors, 2 * width), f32),
                pltpu.VMEM((OUT_PIECES, held) + o_item, f32),
                pltpu.VMEM((OUT_PIECES, held) + o_item, f32),
                pltpu.VMEM((OUT_PIECES, held) + o_item, f32),
            ] + [pltpu.SemaphoreType.DMA((2, pieces))] * 4
            + [pltpu.SemaphoreType.DMA((2, OUT_PIECES))] * 4,
            compiler_params=pltpu.CompilerParams(
                collective_id=m, has_side_effects=True, vmem_limit_bytes=48 * 1024 * 1024
            ),
        )

    branches = [run(m) for m in range(1, half + 1)]
    projected = lax.switch(jnp.maximum(count, 1) - 1, branches, table, e_view, s_view)
    projected = projected.reshape(held, rows, 2, spins, sources)
    first = lax.axis_index("src") * sources
    place = (source_ids[None, :] - first) == jnp.arange(sources, dtype=jnp.int32)[:, None]
    return jnp.einsum(
        "jn,rkpsn->rpsjk", place.astype(f32), projected, precision=lax.Precision.HIGHEST
    )


def solution(mesh):
    in_specs = (
        P("src", "ta", None, "job", None, "xyz"),
        P("ta", "job", None, None, "xyz"),
        P(),
        P("src"),
    )
    out_specs = P("ta", None, "job", "src", "xyz")
    n = mesh.shape["ta"]
    line = n == 4 and mesh.shape["src"] == 2 and mesh.shape["xyz"] == 2
    local = functools.partial(local_line, n) if line else local_general
    return jax.shard_map(local, mesh=mesh, in_specs=in_specs, out_specs=out_specs, check_vma=False)
```

```python
import functools

import jax
import jax.numpy as jnp
from jax import lax
from jax.experimental import pallas as pl
from jax.experimental.pallas import tpu as pltpu
from jax.sharding import PartitionSpec as P

MESH = pl.DeviceIdType.MESH
OUT_PIECES = 4
ROW_CUTS = 2
LANES = 128
SUBLANES = 8


def contract_pair(vectors, spinor):
    vector_real = vectors[:, :, 0]
    vector_imag = vectors[:, :, 1]
    spinor_real = spinor[:, :, 0]
    spinor_imag = spinor[:, :, 1]

    def contract(left_side, right_side):
        return jnp.einsum(
            "tkcx,ntscx->tsnk", left_side, right_side, precision=lax.Precision.HIGHEST
        )

    real_part = contract(vector_real, spinor_real) + contract(vector_imag, spinor_imag)
    imag_part = contract(vector_real, spinor_imag) - contract(vector_imag, spinor_real)
    return jnp.stack([real_part, imag_part], axis=1)


def local_general(spinors, eigvecs, group_of, source_ids):
    extent = group_of.shape[0]
    sort_keys = group_of * extent + jnp.arange(extent, dtype=jnp.int32)
    ordering = jnp.argsort(sort_keys)
    spread = lax.all_to_all(spinors, "ta", split_axis=0, concat_axis=1, tiled=True)
    grouped = jnp.take(spread, ordering, axis=1)
    regrouped = lax.all_to_all(grouped, "ta", split_axis=1, concat_axis=0, tiled=True)
    partial_sums = contract_pair(eigvecs, regrouped)
    summed = lax.psum_scatter(partial_sums, "xyz", scatter_dimension=4, tiled=True)
    inverse = jnp.argsort(source_ids)
    return jnp.take(summed, inverse, axis=3)


def copy_to(src, dst, sems, index, where):
    return pltpu.make_async_remote_copy(
        src_ref=src,
        dst_ref=dst,
        send_sem=sems.at[0, index],
        recv_sem=sems.at[1, index],
        device_id=where,
        device_id_type=MESH,
    )


def routes(words, which, wanted, goes_to, right, m, spots):
    extent = len(wanted)
    half = extent // 2
    crosses, slot = [], []
    for item in range(extent):
        over = goes_to[item] >= half if item < half else goes_to[item] < half
        crosses.append(jnp.where(over, 1, 0))
        slot.append(sum(crosses[item // half * half:item], jnp.int32(0)))
        words[which, 0, item] = wanted[item]
        words[which, 1, item] = slot[item]
    mine = [jnp.where(right == 1, crosses[half + i], crosses[i]) for i in range(half)]
    mine_slot = [jnp.where(right == 1, slot[half + i], slot[i]) for i in range(half)]
    send = []
    for place in range(m):
        at = jnp.int32(0)
        for i in range(half):
            at = at + jnp.where(mine_slot[i] == place, i * mine[i], 0)
        send.append(at)

    def pick(q):
        want = words[which, 0, right * half + q]
        own = jnp.where(want >= half, 1, 0) == right
        near = jnp.where(own, want - right * half, 0)
        far = jnp.where(own, 0, words[which, 1, want])
        return near, jnp.minimum(far, m - 1), own

    return send, [[pick(q) for q in group] for group in spots]


def sites_apart(value):
    pairs = value.reshape(value.shape[0] // 2, 2, SUBLANES, LANES)
    even, odd = pairs[:, 0], pairs[:, 1]
    upper = lax.broadcasted_iota(jnp.int32, even.shape, 1) < SUBLANES // 2
    shift = SUBLANES // 2
    first = jnp.where(upper, even, pltpu.roll(odd, shift, 1))
    second = jnp.where(upper, pltpu.roll(even, shift, 1), odd)
    return first.reshape(-1, LANES), second.reshape(-1, LANES)


def kernel(n, m, pieces, group_ref, e_ref, s_ref, out_ref, *scratch):
    held = e_ref.shape[0]
    scratch = list(scratch)

    def take(count):
        got = scratch[:count]
        del scratch[:count]
        return got

    side_e, mid_e, recv_e, give_e = take(pieces), take(pieces), take(pieces), take(pieces)
    side_o, mid_o, recv_o, give_o = (
        take(OUT_PIECES), take(OUT_PIECES), take(OUT_PIECES), take(OUT_PIECES)
    )
    full, high, low, acc, x_recv, o_recv, o_send, spin_raw, words = take(9)
    in_e, cross_e, back_e, core_e, x_sem, in_o, cross_o, back_o, s_sem = take(9)

    load_s = pltpu.make_async_copy(s_ref, spin_raw, s_sem)
    load_s.start()

    z = lax.axis_index("ta")
    core = lax.axis_index("src")
    xi = lax.axis_index("xyz")
    right = z // (n // 2)
    inner = jnp.logical_and(z > 0, z < n - 1)
    outer = jnp.logical_not(inner)
    to_inner = {"ta": 1 + right}
    to_outer = {"ta": right * (n - 1)}
    to_other = {"ta": n - 1 - z}
    to_core = {"src": 1 - core}
    to_x = {"xyz": 1 - xi}
    outer_at = right * held
    own_at = (1 - right) * held
    depth = e_ref.shape[2] // 2
    cut = depth // ROW_CUTS

    def rows_at(who, i):
        at = who * depth + i % ROW_CUTS * cut
        return i // ROW_CUTS, slice(None), pl.ds(pl.multiple_of(at, cut), cut), slice(None)

    def mine_at(i):
        j, _, rows_, _ = rows_at(core, i)
        return slice(None), j, rows_, slice(None)

    barrier = pltpu.get_barrier_semaphore()
    for where in (to_core, to_x):
        pl.semaphore_signal(barrier, inc=1, device_id=where, device_id_type=MESH)

    @pl.when(inner)
    def _():
        for where in (to_outer, to_other):
            pl.semaphore_signal(barrier, inc=1, device_id=where, device_id_type=MESH)
        pl.semaphore_wait(barrier, 4)

    @pl.when(outer)
    def _():
        pl.semaphore_signal(barrier, inc=1, device_id=to_inner, device_id_type=MESH)
        pl.semaphore_wait(barrier, 3)

    def inward_e(i):
        return copy_to(
            e_ref.at[mine_at(i)], side_e[i].at[pl.ds(outer_at, held)], in_e, i, to_inner
        )

    def across_e(i):
        return copy_to(mid_e[i], recv_e[i], cross_e, i, to_other)

    def back_out_e(i):
        return copy_to(give_e[i], full.at[rows_at(core, i)], back_e, i, to_outer)

    def swap_e(i):
        view = full.at[rows_at(core, i)]
        return copy_to(view, view, core_e, i, to_core)

    def swapped_e(i):
        view = full.at[rows_at(1 - core, i)]
        return copy_to(view, view, core_e, i, to_core)

    def chosen(pick, side, recv):
        near, far, own = pick
        return jnp.where(own, side[near], recv[far])

    @pl.when(outer)
    def _():
        for j in range(pieces):
            inward_e(j).start()

    @pl.when(inner)
    def _():
        for j in range(pieces):
            side_e[j][pl.ds(own_at, held)] = e_ref[mine_at(j)]

    extent = n * held
    group = [group_ref[t] for t in range(extent)]
    rank, ordering = [], []
    for t in range(extent):
        before = sum((jnp.where(group[u] == group[t], 1, 0) for u in range(t)), jnp.int32(0))
        rank.append(group[t] * held + before)
    for r in range(extent):
        ordering.append(
            sum((jnp.where(rank[t] == r, t, 0) for t in range(extent)), jnp.int32(0))
        )
    spots = [[outer_at + i for i in range(held)], [own_at + i for i in range(held)]]
    send_e, (outer_e, own_e) = routes(words, 0, rank, ordering, right, m, spots)
    send_o, (outer_o, own_o) = routes(words, 1, ordering, rank, right, m, spots)

    def split(value):
        top = value.astype(jnp.bfloat16)
        return top, (value - top.astype(jnp.float32)).astype(jnp.bfloat16)

    load_s.wait()
    width = acc.shape[2] // 2
    for t in range(held):
        acc[t] = jnp.zeros(acc.shape[1:], jnp.float32)
        for c in range(high.shape[1] // 2):
            reals = sites_apart(spin_raw[:, t, 0, c])
            imags = sites_apart(spin_raw[:, t, 1, c])
            for tile, (real_, imag_) in enumerate(zip(reals, imags)):
                at = slice(tile * LANES, (tile + 1) * LANES)
                for keep, real, imag in zip((high, low), split(real_), split(imag_)):
                    keep[t, 2 * c, :width, at] = real
                    keep[t, 2 * c, width:, at] = imag
                    keep[t, 2 * c + 1, :width, at] = imag
                    keep[t, 2 * c + 1, width:, at] = -real

    def dot(a, b):
        return lax.dot_general(
            a, b, (((1,), (1,)), ((), ())), preferred_element_type=jnp.float32
        )

    def contract(j):
        for t in range(held):
            top, rest = split(full[j, t])
            acc[t] += dot(top, high[t, j]) + (dot(top, low[t, j]) + dot(rest, high[t, j]))

    for tick in range(pieces + 3):
        i, before, late = tick, tick - 1, tick - 2

        @pl.when(inner)
        def _():
            if i < pieces:
                inward_e(i).wait_recv()
                for slot in range(m):
                    mid_e[i][slot] = side_e[i][send_e[slot]]
                across_e(i).start()
            if 0 <= before < pieces:
                across_e(before).wait_recv()
                for k in range(held):
                    give_e[before][k] = chosen(outer_e[k], side_e[before], recv_e[before])
                back_out_e(before).start()
                j, _, rows_, _ = rows_at(core, before)
                for k in range(held):
                    full[j, k, rows_, :] = chosen(own_e[k], side_e[before], recv_e[before])
                swap_e(before).start()

        if 0 <= late < pieces:
            @pl.when(outer)
            def _():
                back_out_e(late).wait_recv()
                swap_e(late).start()

        last = tick - 3
        if last >= 0:
            swapped_e(last).wait_recv()
            if last % ROW_CUTS == ROW_CUTS - 1:
                contract(last // ROW_CUTS)

    for i in range(pieces):
        swap_e(i).wait_send()

    @pl.when(inner)
    def _():
        for i in range(pieces):
            across_e(i).wait_send()
            back_out_e(i).wait_send()

    @pl.when(outer)
    def _():
        for i in range(pieces):
            inward_e(i).wait_send()

    rows = acc.shape[1] // 2
    part = rows // OUT_PIECES

    def x_swap(q):
        there = pl.ds(pl.multiple_of((1 - xi) * rows + q * part, part), part)
        return copy_to(acc.at[:, there, :], x_recv.at[q], x_sem, q, to_x)

    def summed(q):
        here = pl.ds(pl.multiple_of(xi * rows + q * part, part), part)
        return acc[:, here, :] + x_recv[q]

    def inward_o(q):
        return copy_to(o_send.at[q], side_o[q].at[pl.ds(outer_at, held)], in_o, q, to_inner)

    def across_o(q):
        return copy_to(mid_o[q], recv_o[q], cross_o, q, to_other)

    def back_out_o(q):
        return copy_to(give_o[q], o_recv.at[q], back_o, q, to_outer)

    for q in range(OUT_PIECES):
        x_swap(q).start()

    @pl.when(outer)
    def _():
        for q in range(OUT_PIECES):
            x_swap(q).wait_recv()
            o_send[q] = summed(q)
            inward_o(q).start()
        for q in range(OUT_PIECES):
            back_out_o(q).wait_recv()
            out_ref[:, q * part:(q + 1) * part, :] = o_recv[q]
        for q in range(OUT_PIECES):
            inward_o(q).wait_send()

    @pl.when(inner)
    def _():
        for q in range(OUT_PIECES):
            x_swap(q).wait_recv()
            side_o[q][pl.ds(own_at, held)] = summed(q)
        for q in range(OUT_PIECES):
            inward_o(q).wait_recv()
            for slot in range(m):
                mid_o[q][slot] = side_o[q][send_o[slot]]
            across_o(q).start()
        for q in range(OUT_PIECES):
            across_o(q).wait_recv()
            for i in range(held):
                give_o[q][i] = chosen(outer_o[i], side_o[q], recv_o[q])
            back_out_o(q).start()
            for i in range(held):
                out_ref[i, q * part:(q + 1) * part, :] = chosen(own_o[i], side_o[q], recv_o[q])
        for q in range(OUT_PIECES):
            across_o(q).wait_send()
            back_out_o(q).wait_send()

    for q in range(OUT_PIECES):
        x_swap(q).wait_send()


def local_line(n, spinors, eigvecs, group_of, source_ids):
    extent = group_of.shape[0]
    half = extent // 2
    sources, held, _, spins, colours, sites = spinors.shape
    vectors = eigvecs.shape[1]
    layers = 2 * colours
    pieces = layers * ROW_CUTS
    depth = vectors // 2
    width = spins * sources

    count = jnp.sum((group_of[:half] >= n // 2).astype(jnp.int32))

    e_view = eigvecs.transpose(0, 3, 2, 1, 4).reshape(held, layers, vectors, sites)
    tiled = spinors.reshape(sources, held, 2, spins, colours, sites // LANES, LANES)
    s_view = tiled.transpose(0, 1, 2, 4, 5, 3, 6).reshape(
        sources, held, 2, colours, SUBLANES, LANES
    )

    rows = vectors // 2
    part = rows // OUT_PIECES
    f32 = jnp.float32

    def run(m):
        vmem = pl.BlockSpec(memory_space=pltpu.VMEM)
        e_item = (depth // ROW_CUTS, sites)
        o_item = (part, 2 * width)
        buffers = []
        for count_, item in ((pieces, e_item), (OUT_PIECES, o_item)):
            for slots in (half, m, m, held):
                buffers += [pltpu.VMEM((slots,) + item, f32)] * count_
        return pl.pallas_call(
            functools.partial(kernel, n, m, pieces),
            name=f"project_{m}",
            out_shape=jax.ShapeDtypeStruct((held, rows, 2 * width), f32),
            in_specs=[
                pl.BlockSpec(memory_space=pltpu.SMEM), vmem, pl.BlockSpec(memory_space=pl.ANY)
            ],
            out_specs=vmem,
            scratch_shapes=buffers + [
                pltpu.VMEM((layers, held, vectors, sites), f32),
                pltpu.VMEM((held, layers, 2 * width, sites), jnp.bfloat16),
                pltpu.VMEM((held, layers, 2 * width, sites), jnp.bfloat16),
                pltpu.VMEM((held, vectors, 2 * width), f32),
                pltpu.VMEM((OUT_PIECES, held) + o_item, f32),
                pltpu.VMEM((OUT_PIECES, held) + o_item, f32),
                pltpu.VMEM((OUT_PIECES, held) + o_item, f32),
                pltpu.VMEM(s_view.shape, f32),
                pltpu.SMEM((2, 2, extent), jnp.int32),
            ] + [pltpu.SemaphoreType.DMA((2, pieces))] * 4
            + [pltpu.SemaphoreType.DMA((2, OUT_PIECES))] * 4 + [pltpu.SemaphoreType.DMA],
            compiler_params=pltpu.CompilerParams(
                collective_id=m, has_side_effects=True, vmem_limit_bytes=48 * 1024 * 1024
            ),
        )

    branches = [run(m) for m in range(1, half + 1)]
    projected = lax.switch(jnp.maximum(count, 1) - 1, branches, group_of, e_view, s_view)
    projected = projected.reshape(held, rows, 2, sources, spins)
    first = lax.axis_index("src") * sources
    place = (source_ids[None, :] - first) == jnp.arange(sources, dtype=jnp.int32)[:, None]
    return jnp.einsum(
        "jn,rkpns->rpsjk", place.astype(f32), projected, precision=lax.Precision.HIGHEST
    )


def solution(mesh):
    in_specs = (
        P("src", "ta", None, "job", None, "xyz"),
        P("ta", "job", None, None, "xyz"),
        P(),
        P("src"),
    )
    out_specs = P("ta", None, "job", "src", "xyz")
    n = mesh.shape["ta"]
    line = n == 4 and mesh.shape["src"] == 2 and mesh.shape["xyz"] == 2

    def local(spinors, eigvecs, group_of, source_ids):
        tiles = spinors.shape[5] // LANES
        if line and tiles == 2 and tiles * spinors.shape[3] == SUBLANES:
            return local_line(n, spinors, eigvecs, group_of, source_ids)
        return local_general(spinors, eigvecs, group_of, source_ids)

    return jax.shard_map(local, mesh=mesh, in_specs=in_specs, out_specs=out_specs, check_vma=False)
```

```python
import functools

import jax
import jax.numpy as jnp
from jax import lax
from jax.experimental import pallas as pl
from jax.experimental.pallas import tpu as pltpu
from jax.sharding import PartitionSpec as P

MESH = pl.DeviceIdType.MESH
OUT_PIECES = 4
PIECE_LAYERS = 1
LANES = 128
SUBLANES = 8


def contract_pair(vectors, spinor):
    vector_real = vectors[:, :, 0]
    vector_imag = vectors[:, :, 1]
    spinor_real = spinor[:, :, 0]
    spinor_imag = spinor[:, :, 1]

    def contract(left_side, right_side):
        return jnp.einsum(
            "tkcx,ntscx->tsnk", left_side, right_side, precision=lax.Precision.HIGHEST
        )

    real_part = contract(vector_real, spinor_real) + contract(vector_imag, spinor_imag)
    imag_part = contract(vector_real, spinor_imag) - contract(vector_imag, spinor_real)
    return jnp.stack([real_part, imag_part], axis=1)


def local_general(spinors, eigvecs, group_of, source_ids):
    extent = group_of.shape[0]
    sort_keys = group_of * extent + jnp.arange(extent, dtype=jnp.int32)
    ordering = jnp.argsort(sort_keys)
    spread = lax.all_to_all(spinors, "ta", split_axis=0, concat_axis=1, tiled=True)
    grouped = jnp.take(spread, ordering, axis=1)
    regrouped = lax.all_to_all(grouped, "ta", split_axis=1, concat_axis=0, tiled=True)
    partial_sums = contract_pair(eigvecs, regrouped)
    summed = lax.psum_scatter(partial_sums, "xyz", scatter_dimension=4, tiled=True)
    inverse = jnp.argsort(source_ids)
    return jnp.take(summed, inverse, axis=3)


def copy_to(src, dst, sems, index, where):
    return pltpu.make_async_remote_copy(
        src_ref=src,
        dst_ref=dst,
        send_sem=sems.at[0, index],
        recv_sem=sems.at[1, index],
        device_id=where,
        device_id_type=MESH,
    )


def routes(words, which, wanted, goes_to, right, m, spots):
    extent = len(wanted)
    half = extent // 2
    crosses, slot = [], []
    for item in range(extent):
        over = goes_to[item] >= half if item < half else goes_to[item] < half
        crosses.append(jnp.where(over, 1, 0))
        slot.append(sum(crosses[item // half * half:item], jnp.int32(0)))
        words[which, 0, item] = wanted[item]
        words[which, 1, item] = slot[item]
    mine = [jnp.where(right == 1, crosses[half + i], crosses[i]) for i in range(half)]
    mine_slot = [jnp.where(right == 1, slot[half + i], slot[i]) for i in range(half)]
    send = []
    for place in range(m):
        at = jnp.int32(0)
        for i in range(half):
            at = at + jnp.where(mine_slot[i] == place, i * mine[i], 0)
        send.append(at)

    def pick(q):
        want = words[which, 0, right * half + q]
        own = jnp.where(want >= half, 1, 0) == right
        near = jnp.where(own, want - right * half, 0)
        far = jnp.where(own, 0, words[which, 1, want])
        return near, jnp.minimum(far, m - 1), own

    return send, [[pick(q) for q in group] for group in spots]


def sites_apart(value):
    pairs = value.reshape(value.shape[0] // 2, 2, SUBLANES, LANES)
    even, odd = pairs[:, 0], pairs[:, 1]
    upper = lax.broadcasted_iota(jnp.int32, even.shape, 1) < SUBLANES // 2
    shift = SUBLANES // 2
    first = jnp.where(upper, even, pltpu.roll(odd, shift, 1))
    second = jnp.where(upper, pltpu.roll(even, shift, 1), odd)
    return first.reshape(-1, LANES), second.reshape(-1, LANES)


def kernel(n, m, plan, group_ref, e_ref, s_ref, out_ref, *scratch):
    held = e_ref.shape[0]
    pieces = len(plan)
    scratch = list(scratch)

    def take(count):
        got = scratch[:count]
        del scratch[:count]
        return got

    side_e, mid_e, recv_e, give_e = take(pieces), take(pieces), take(pieces), take(pieces)
    side_o, mid_o, recv_o, give_o = (
        take(OUT_PIECES), take(OUT_PIECES), take(OUT_PIECES), take(OUT_PIECES)
    )
    full, high, low, acc, x_recv, o_recv, o_send, spin_raw, words = take(9)
    in_e, cross_e, back_e, core_e, x_sem, in_o, cross_o, back_o, s_sem = take(9)

    load_s = pltpu.make_async_copy(s_ref, spin_raw, s_sem)
    load_s.start()

    z = lax.axis_index("ta")
    core = lax.axis_index("src")
    xi = lax.axis_index("xyz")
    right = z // (n // 2)
    inner = jnp.logical_and(z > 0, z < n - 1)
    outer = jnp.logical_not(inner)
    to_inner = {"ta": 1 + right}
    to_outer = {"ta": right * (n - 1)}
    to_other = {"ta": n - 1 - z}
    to_core = {"src": 1 - core}
    to_x = {"xyz": 1 - xi}
    outer_at = right * held
    own_at = (1 - right) * held
    depth = e_ref.shape[2] // 2

    def rows_at(who, i):
        first, count = plan[i]
        at = pl.multiple_of(who * depth, depth)
        return slice(None), pl.ds(first, count), pl.ds(at, depth), slice(None)

    def mine_at(i):
        return rows_at(core, i)

    barrier = pltpu.get_barrier_semaphore()
    for where in (to_core, to_x):
        pl.semaphore_signal(barrier, inc=1, device_id=where, device_id_type=MESH)

    @pl.when(inner)
    def _():
        for where in (to_outer, to_other):
            pl.semaphore_signal(barrier, inc=1, device_id=where, device_id_type=MESH)
        pl.semaphore_wait(barrier, 4)

    @pl.when(outer)
    def _():
        pl.semaphore_signal(barrier, inc=1, device_id=to_inner, device_id_type=MESH)
        pl.semaphore_wait(barrier, 3)

    def inward_e(i):
        return copy_to(
            e_ref.at[mine_at(i)], side_e[i].at[pl.ds(outer_at, held)], in_e, i, to_inner
        )

    def across_e(i):
        return copy_to(mid_e[i], recv_e[i], cross_e, i, to_other)

    def back_out_e(i):
        return copy_to(give_e[i], full.at[rows_at(core, i)], back_e, i, to_outer)

    def swap_e(i):
        view = full.at[rows_at(core, i)]
        return copy_to(view, view, core_e, i, to_core)

    def swapped_e(i):
        view = full.at[rows_at(1 - core, i)]
        return copy_to(view, view, core_e, i, to_core)

    def chosen(pick, side, recv):
        near, far, own = pick
        return jnp.where(own, side[near], recv[far])

    @pl.when(outer)
    def _():
        for j in range(pieces):
            inward_e(j).start()

    @pl.when(inner)
    def _():
        for j in range(pieces):
            side_e[j][pl.ds(own_at, held)] = e_ref[mine_at(j)]

    extent = n * held
    group = [group_ref[t] for t in range(extent)]
    rank, ordering = [], []
    for t in range(extent):
        before = sum((jnp.where(group[u] == group[t], 1, 0) for u in range(t)), jnp.int32(0))
        rank.append(group[t] * held + before)
    for r in range(extent):
        ordering.append(
            sum((jnp.where(rank[t] == r, t, 0) for t in range(extent)), jnp.int32(0))
        )
    spots = [[outer_at + i for i in range(held)], [own_at + i for i in range(held)]]
    send_e, (outer_e, own_e) = routes(words, 0, rank, ordering, right, m, spots)
    send_o, (outer_o, own_o) = routes(words, 1, ordering, rank, right, m, spots)

    def split(value):
        top = value.astype(jnp.bfloat16)
        return top, (value - top.astype(jnp.float32)).astype(jnp.bfloat16)

    load_s.wait()
    width = acc.shape[2] // 2
    for t in range(held):
        acc[t] = jnp.zeros(acc.shape[1:], jnp.float32)
        for c in range(high.shape[1] // 2):
            reals = sites_apart(spin_raw[:, t, 0, c])
            imags = sites_apart(spin_raw[:, t, 1, c])
            for tile, (real_, imag_) in enumerate(zip(reals, imags)):
                at = slice(tile * LANES, (tile + 1) * LANES)
                for keep, real, imag in zip((high, low), split(real_), split(imag_)):
                    keep[t, 2 * c, :width, at] = real
                    keep[t, 2 * c, width:, at] = imag
                    keep[t, 2 * c + 1, :width, at] = imag
                    keep[t, 2 * c + 1, width:, at] = -real

    def dot(a, b):
        return lax.dot_general(
            a, b, (((1,), (1,)), ((), ())), preferred_element_type=jnp.float32
        )

    def contract(j):
        for t in range(held):
            top, rest = split(full[t, j])
            acc[t] += dot(top, high[t, j]) + (dot(top, low[t, j]) + dot(rest, high[t, j]))

    for tick in range(pieces + 3):
        i, before, late = tick, tick - 1, tick - 2

        @pl.when(inner)
        def _():
            if i < pieces:
                inward_e(i).wait_recv()
                for slot in range(m):
                    mid_e[i][slot] = side_e[i][send_e[slot]]
                across_e(i).start()
            if 0 <= before < pieces:
                across_e(before).wait_recv()
                for k in range(held):
                    give_e[before][k] = chosen(outer_e[k], side_e[before], recv_e[before])
                back_out_e(before).start()
                _, layers_, rows_, _ = rows_at(core, before)
                for k in range(held):
                    full[k, layers_, rows_, :] = chosen(own_e[k], side_e[before], recv_e[before])
                swap_e(before).start()

        if 0 <= late < pieces:
            @pl.when(outer)
            def _():
                back_out_e(late).wait_recv()
                swap_e(late).start()

        last = tick - 3
        if last >= 0:
            swapped_e(last).wait_recv()
            for layer in range(plan[last][0], sum(plan[last])):
                contract(layer)

    for i in range(pieces):
        swap_e(i).wait_send()

    @pl.when(inner)
    def _():
        for i in range(pieces):
            across_e(i).wait_send()
            back_out_e(i).wait_send()

    @pl.when(outer)
    def _():
        for i in range(pieces):
            inward_e(i).wait_send()

    rows = acc.shape[1] // 2
    part = rows // OUT_PIECES

    def x_swap(q):
        there = pl.ds(pl.multiple_of((1 - xi) * rows + q * part, part), part)
        return copy_to(acc.at[:, there, :], x_recv.at[q], x_sem, q, to_x)

    def summed(q):
        here = pl.ds(pl.multiple_of(xi * rows + q * part, part), part)
        return acc[:, here, :] + x_recv[q]

    def inward_o(q):
        return copy_to(o_send.at[q], side_o[q].at[pl.ds(outer_at, held)], in_o, q, to_inner)

    def across_o(q):
        return copy_to(mid_o[q], recv_o[q], cross_o, q, to_other)

    def back_out_o(q):
        return copy_to(give_o[q], o_recv.at[q], back_o, q, to_outer)

    for q in range(OUT_PIECES):
        x_swap(q).start()

    @pl.when(outer)
    def _():
        for q in range(OUT_PIECES):
            x_swap(q).wait_recv()
            o_send[q] = summed(q)
            inward_o(q).start()
        for q in range(OUT_PIECES):
            back_out_o(q).wait_recv()
            out_ref[:, q * part:(q + 1) * part, :] = o_recv[q]
        for q in range(OUT_PIECES):
            inward_o(q).wait_send()

    @pl.when(inner)
    def _():
        for q in range(OUT_PIECES):
            x_swap(q).wait_recv()
            side_o[q][pl.ds(own_at, held)] = summed(q)
        for q in range(OUT_PIECES):
            inward_o(q).wait_recv()
            for slot in range(m):
                mid_o[q][slot] = side_o[q][send_o[slot]]
            across_o(q).start()
        for q in range(OUT_PIECES):
            across_o(q).wait_recv()
            for i in range(held):
                give_o[q][i] = chosen(outer_o[i], side_o[q], recv_o[q])
            back_out_o(q).start()
            for i in range(held):
                out_ref[i, q * part:(q + 1) * part, :] = chosen(own_o[i], side_o[q], recv_o[q])
        for q in range(OUT_PIECES):
            across_o(q).wait_send()
            back_out_o(q).wait_send()

    for q in range(OUT_PIECES):
        x_swap(q).wait_send()


def local_line(n, spinors, eigvecs, group_of, source_ids):
    extent = group_of.shape[0]
    half = extent // 2
    sources, held, _, spins, colours, sites = spinors.shape
    vectors = eigvecs.shape[1]
    layers = 2 * colours
    plan = [
        (first, min(PIECE_LAYERS, layers - first)) for first in range(0, layers, PIECE_LAYERS)
    ]
    depth = vectors // 2
    width = spins * sources

    count = jnp.sum((group_of[:half] >= n // 2).astype(jnp.int32))

    e_view = eigvecs.transpose(0, 3, 2, 1, 4).reshape(held, layers, vectors, sites)
    tiled = spinors.reshape(sources, held, 2, spins, colours, sites // LANES, LANES)
    s_view = tiled.transpose(0, 1, 2, 4, 5, 3, 6).reshape(
        sources, held, 2, colours, SUBLANES, LANES
    )

    rows = vectors // 2
    part = rows // OUT_PIECES
    f32 = jnp.float32

    def run(m):
        vmem = pl.BlockSpec(memory_space=pltpu.VMEM)
        e_items = [(size, depth, sites) for _, size in plan]
        o_item = (part, 2 * width)
        buffers = []
        for pieces_ in (e_items, [o_item] * OUT_PIECES):
            for slots in (half, m, m, held):
                buffers += [pltpu.VMEM((slots,) + item, f32) for item in pieces_]
        return pl.pallas_call(
            functools.partial(kernel, n, m, plan),
            name=f"project_{m}",
            out_shape=jax.ShapeDtypeStruct((held, rows, 2 * width), f32),
            in_specs=[
                pl.BlockSpec(memory_space=pltpu.SMEM), vmem, pl.BlockSpec(memory_space=pl.ANY)
            ],
            out_specs=vmem,
            scratch_shapes=buffers + [
                pltpu.VMEM((held, layers, vectors, sites), f32),
                pltpu.VMEM((held, layers, 2 * width, sites), jnp.bfloat16),
                pltpu.VMEM((held, layers, 2 * width, sites), jnp.bfloat16),
                pltpu.VMEM((held, vectors, 2 * width), f32),
                pltpu.VMEM((OUT_PIECES, held) + o_item, f32),
                pltpu.VMEM((OUT_PIECES, held) + o_item, f32),
                pltpu.VMEM((OUT_PIECES, held) + o_item, f32),
                pltpu.VMEM(s_view.shape, f32),
                pltpu.SMEM((2, 2, extent), jnp.int32),
            ] + [pltpu.SemaphoreType.DMA((2, len(plan)))] * 4
            + [pltpu.SemaphoreType.DMA((2, OUT_PIECES))] * 4 + [pltpu.SemaphoreType.DMA],
            compiler_params=pltpu.CompilerParams(
                collective_id=m, has_side_effects=True, vmem_limit_bytes=48 * 1024 * 1024
            ),
        )

    branches = [run(m) for m in range(1, half + 1)]
    projected = lax.switch(jnp.maximum(count, 1) - 1, branches, group_of, e_view, s_view)
    projected = projected.reshape(held, rows, 2, sources, spins)
    first = lax.axis_index("src") * sources
    place = (source_ids[None, :] - first) == jnp.arange(sources, dtype=jnp.int32)[:, None]
    return jnp.einsum(
        "jn,rkpns->rpsjk", place.astype(f32), projected, precision=lax.Precision.HIGHEST
    )


def solution(mesh):
    in_specs = (
        P("src", "ta", None, "job", None, "xyz"),
        P("ta", "job", None, None, "xyz"),
        P(),
        P("src"),
    )
    out_specs = P("ta", None, "job", "src", "xyz")
    n = mesh.shape["ta"]
    line = n == 4 and mesh.shape["src"] == 2 and mesh.shape["xyz"] == 2

    def local(spinors, eigvecs, group_of, source_ids):
        tiles = spinors.shape[5] // LANES
        if line and tiles == 2 and tiles * spinors.shape[3] == SUBLANES:
            return local_line(n, spinors, eigvecs, group_of, source_ids)
        return local_general(spinors, eigvecs, group_of, source_ids)

    return jax.shard_map(local, mesh=mesh, in_specs=in_specs, out_specs=out_specs, check_vma=False)
```

```python
import functools

import jax
import jax.numpy as jnp
from jax import lax
from jax.experimental import pallas as pl
from jax.experimental.pallas import tpu as pltpu
from jax.sharding import PartitionSpec as P

MESH = pl.DeviceIdType.MESH
OUT_PIECES = 8
PIECE_LAYERS = 1
LANES = 128
SUBLANES = 8


def contract_pair(vectors, spinor):
    vector_real = vectors[:, :, 0]
    vector_imag = vectors[:, :, 1]
    spinor_real = spinor[:, :, 0]
    spinor_imag = spinor[:, :, 1]

    def contract(left_side, right_side):
        return jnp.einsum(
            "tkcx,ntscx->tsnk", left_side, right_side, precision=lax.Precision.HIGHEST
        )

    real_part = contract(vector_real, spinor_real) + contract(vector_imag, spinor_imag)
    imag_part = contract(vector_real, spinor_imag) - contract(vector_imag, spinor_real)
    return jnp.stack([real_part, imag_part], axis=1)


def local_general(spinors, eigvecs, group_of, source_ids):
    extent = group_of.shape[0]
    sort_keys = group_of * extent + jnp.arange(extent, dtype=jnp.int32)
    ordering = jnp.argsort(sort_keys)
    spread = lax.all_to_all(spinors, "ta", split_axis=0, concat_axis=1, tiled=True)
    grouped = jnp.take(spread, ordering, axis=1)
    regrouped = lax.all_to_all(grouped, "ta", split_axis=1, concat_axis=0, tiled=True)
    partial_sums = contract_pair(eigvecs, regrouped)
    summed = lax.psum_scatter(partial_sums, "xyz", scatter_dimension=4, tiled=True)
    inverse = jnp.argsort(source_ids)
    return jnp.take(summed, inverse, axis=3)


def copy_to(src, dst, sems, index, where):
    return pltpu.make_async_remote_copy(
        src_ref=src,
        dst_ref=dst,
        send_sem=sems.at[0, index],
        recv_sem=sems.at[1, index],
        device_id=where,
        device_id_type=MESH,
    )


def routes(words, which, wanted, goes_to, right, m, spots):
    extent = len(wanted)
    half = extent // 2
    crosses, slot = [], []
    for item in range(extent):
        over = goes_to[item] >= half if item < half else goes_to[item] < half
        crosses.append(jnp.where(over, 1, 0))
        slot.append(sum(crosses[item // half * half:item], jnp.int32(0)))
        words[which, 0, item] = wanted[item]
        words[which, 1, item] = slot[item]
    mine = [jnp.where(right == 1, crosses[half + i], crosses[i]) for i in range(half)]
    mine_slot = [jnp.where(right == 1, slot[half + i], slot[i]) for i in range(half)]
    send = []
    for place in range(m):
        at = jnp.int32(0)
        for i in range(half):
            at = at + jnp.where(mine_slot[i] == place, i * mine[i], 0)
        send.append(at)

    def pick(q):
        want = words[which, 0, right * half + q]
        own = jnp.where(want >= half, 1, 0) == right
        near = jnp.where(own, want - right * half, 0)
        far = jnp.where(own, 0, words[which, 1, want])
        return near, jnp.minimum(far, m - 1), own

    return send, [[pick(q) for q in group] for group in spots]


def sites_apart(value):
    pairs = value.reshape(value.shape[0] // 2, 2, SUBLANES, LANES)
    even, odd = pairs[:, 0], pairs[:, 1]
    upper = lax.broadcasted_iota(jnp.int32, even.shape, 1) < SUBLANES // 2
    shift = SUBLANES // 2
    first = jnp.where(upper, even, pltpu.roll(odd, shift, 1))
    second = jnp.where(upper, pltpu.roll(even, shift, 1), odd)
    return first.reshape(-1, LANES), second.reshape(-1, LANES)


def kernel(n, m, plan, group_ref, e_ref, s_ref, out_ref, *scratch):
    held = e_ref.shape[0]
    pieces = len(plan)
    scratch = list(scratch)

    def take(count):
        got = scratch[:count]
        del scratch[:count]
        return got

    side_e, mid_e, recv_e, give_e = take(pieces), take(pieces), take(pieces), take(pieces)
    side_o, mid_o, recv_o, give_o = (
        take(OUT_PIECES), take(OUT_PIECES), take(OUT_PIECES), take(OUT_PIECES)
    )
    full, high, low, acc, x_recv, o_recv, o_send, spin_raw, words = take(9)
    in_e, cross_e, back_e, core_e, x_sem, in_o, cross_o, back_o, s_sem = take(9)

    load_s = pltpu.make_async_copy(s_ref, spin_raw, s_sem)
    load_s.start()

    z = lax.axis_index("ta")
    core = lax.axis_index("src")
    xi = lax.axis_index("xyz")
    right = z // (n // 2)
    inner = jnp.logical_and(z > 0, z < n - 1)
    outer = jnp.logical_not(inner)
    to_inner = {"ta": 1 + right}
    to_outer = {"ta": right * (n - 1)}
    to_other = {"ta": n - 1 - z}
    to_core = {"src": 1 - core}
    to_x = {"xyz": 1 - xi}
    outer_at = right * held
    own_at = (1 - right) * held
    depth = e_ref.shape[2] // 2

    def rows_at(who, i):
        first, count = plan[i]
        at = pl.multiple_of(who * depth, depth)
        return slice(None), pl.ds(first, count), pl.ds(at, depth), slice(None)

    def mine_at(i):
        return rows_at(core, i)

    barrier = pltpu.get_barrier_semaphore()
    for where in (to_core, to_x):
        pl.semaphore_signal(barrier, inc=1, device_id=where, device_id_type=MESH)

    @pl.when(inner)
    def _():
        for where in (to_outer, to_other):
            pl.semaphore_signal(barrier, inc=1, device_id=where, device_id_type=MESH)
        pl.semaphore_wait(barrier, 4)

    @pl.when(outer)
    def _():
        pl.semaphore_signal(barrier, inc=1, device_id=to_inner, device_id_type=MESH)
        pl.semaphore_wait(barrier, 3)

    def inward_e(i):
        return copy_to(
            e_ref.at[mine_at(i)], side_e[i].at[pl.ds(outer_at, held)], in_e, i, to_inner
        )

    def across_e(i):
        return copy_to(mid_e[i], recv_e[i], cross_e, i, to_other)

    def back_out_e(i):
        return copy_to(give_e[i], full.at[rows_at(core, i)], back_e, i, to_outer)

    def swap_e(i):
        view = full.at[rows_at(core, i)]
        return copy_to(view, view, core_e, i, to_core)

    def swapped_e(i):
        view = full.at[rows_at(1 - core, i)]
        return copy_to(view, view, core_e, i, to_core)

    def chosen(pick, side, recv):
        near, far, own = pick
        return jnp.where(own, side[near], recv[far])

    @pl.when(outer)
    def _():
        for j in range(pieces):
            inward_e(j).start()

    @pl.when(inner)
    def _():
        for j in range(pieces):
            side_e[j][pl.ds(own_at, held)] = e_ref[mine_at(j)]

    extent = n * held
    group = [group_ref[t] for t in range(extent)]
    rank, ordering = [], []
    for t in range(extent):
        before = sum((jnp.where(group[u] == group[t], 1, 0) for u in range(t)), jnp.int32(0))
        rank.append(group[t] * held + before)
    for r in range(extent):
        ordering.append(
            sum((jnp.where(rank[t] == r, t, 0) for t in range(extent)), jnp.int32(0))
        )
    spots = [[outer_at + i for i in range(held)], [own_at + i for i in range(held)]]
    send_e, (outer_e, own_e) = routes(words, 0, rank, ordering, right, m, spots)
    send_o, (outer_o, own_o) = routes(words, 1, ordering, rank, right, m, spots)

    def split(value):
        top = value.astype(jnp.bfloat16)
        return top, (value - top.astype(jnp.float32)).astype(jnp.bfloat16)

    load_s.wait()
    width = acc.shape[2] // 2
    for t in range(held):
        acc[t] = jnp.zeros(acc.shape[1:], jnp.float32)
        for c in range(high.shape[1] // 2):
            reals = sites_apart(spin_raw[:, t, 0, c])
            imags = sites_apart(spin_raw[:, t, 1, c])
            for tile, (real_, imag_) in enumerate(zip(reals, imags)):
                at = slice(tile * LANES, (tile + 1) * LANES)
                for keep, real, imag in zip((high, low), split(real_), split(imag_)):
                    keep[t, 2 * c, :width, at] = real
                    keep[t, 2 * c, width:, at] = imag
                    keep[t, 2 * c + 1, :width, at] = imag
                    keep[t, 2 * c + 1, width:, at] = -real

    def dot(a, b):
        return lax.dot_general(
            a, b, (((1,), (1,)), ((), ())), preferred_element_type=jnp.float32
        )

    def contract(j):
        for t in range(held):
            top, rest = split(full[t, j])
            acc[t] += dot(top, high[t, j]) + (dot(top, low[t, j]) + dot(rest, high[t, j]))

    layers = high.shape[1]

    def contract_rows(j, at):
        for t in range(held):
            top, rest = split(full[t, j, at, :])
            acc[t, at, :] += dot(top, high[t, j]) + (dot(top, low[t, j]) + dot(rest, high[t, j]))

    for tick in range(pieces + 3):
        i, before, late = tick, tick - 1, tick - 2

        @pl.when(inner)
        def _():
            if i < pieces:
                inward_e(i).wait_recv()
                for slot in range(m):
                    mid_e[i][slot] = side_e[i][send_e[slot]]
                across_e(i).start()
            if 0 <= before < pieces:
                across_e(before).wait_recv()
                for k in range(held):
                    give_e[before][k] = chosen(outer_e[k], side_e[before], recv_e[before])
                back_out_e(before).start()
                _, layers_, rows_, _ = rows_at(core, before)
                for k in range(held):
                    full[k, layers_, rows_, :] = chosen(own_e[k], side_e[before], recv_e[before])
                swap_e(before).start()

        if 0 <= late < pieces:
            @pl.when(outer)
            def _():
                back_out_e(late).wait_recv()
                swap_e(late).start()

        last = tick - 3
        if last >= 0:
            swapped_e(last).wait_recv()
            for layer in range(plan[last][0], min(sum(plan[last]), layers - 1)):
                contract(layer)

    for i in range(pieces):
        swap_e(i).wait_send()

    @pl.when(inner)
    def _():
        for i in range(pieces):
            across_e(i).wait_send()
            back_out_e(i).wait_send()

    @pl.when(outer)
    def _():
        for i in range(pieces):
            inward_e(i).wait_send()

    rows = acc.shape[1] // 2
    part = rows // OUT_PIECES

    def x_swap(q):
        there = pl.ds(pl.multiple_of((1 - xi) * rows + q * part, part), part)
        return copy_to(acc.at[:, there, :], x_recv.at[q], x_sem, q, to_x)

    def summed(q):
        here = pl.ds(pl.multiple_of(xi * rows + q * part, part), part)
        return acc[:, here, :] + x_recv[q]

    def inward_o(q):
        return copy_to(o_send.at[q], side_o[q].at[pl.ds(outer_at, held)], in_o, q, to_inner)

    def across_o(q):
        return copy_to(mid_o[q], recv_o[q], cross_o, q, to_other)

    def back_out_o(q):
        return copy_to(give_o[q], o_recv.at[q], back_o, q, to_outer)

    contract_rows(layers - 1, pl.ds(pl.multiple_of((1 - xi) * rows, rows), rows))
    for q in range(OUT_PIECES):
        x_swap(q).start()
    contract_rows(layers - 1, pl.ds(pl.multiple_of(xi * rows, rows), rows))

    @pl.when(outer)
    def _():
        for q in range(OUT_PIECES):
            x_swap(q).wait_recv()
            o_send[q] = summed(q)
            inward_o(q).start()
        for q in range(OUT_PIECES):
            back_out_o(q).wait_recv()
            out_ref[:, q * part:(q + 1) * part, :] = o_recv[q]
        for q in range(OUT_PIECES):
            inward_o(q).wait_send()

    @pl.when(inner)
    def _():
        for q in range(OUT_PIECES):
            x_swap(q).wait_recv()
            side_o[q][pl.ds(own_at, held)] = summed(q)
        for q in range(OUT_PIECES):
            inward_o(q).wait_recv()
            for slot in range(m):
                mid_o[q][slot] = side_o[q][send_o[slot]]
            across_o(q).start()
        for q in range(OUT_PIECES):
            across_o(q).wait_recv()
            for i in range(held):
                give_o[q][i] = chosen(outer_o[i], side_o[q], recv_o[q])
            back_out_o(q).start()
            for i in range(held):
                out_ref[i, q * part:(q + 1) * part, :] = chosen(own_o[i], side_o[q], recv_o[q])
        for q in range(OUT_PIECES):
            across_o(q).wait_send()
            back_out_o(q).wait_send()

    for q in range(OUT_PIECES):
        x_swap(q).wait_send()


def local_line(n, spinors, eigvecs, group_of, source_ids):
    extent = group_of.shape[0]
    half = extent // 2
    sources, held, _, spins, colours, sites = spinors.shape
    vectors = eigvecs.shape[1]
    layers = 2 * colours
    plan = [
        (first, min(PIECE_LAYERS, layers - first)) for first in range(0, layers, PIECE_LAYERS)
    ]
    depth = vectors // 2
    width = spins * sources

    count = jnp.sum((group_of[:half] >= n // 2).astype(jnp.int32))

    e_view = eigvecs.transpose(0, 3, 2, 1, 4).reshape(held, layers, vectors, sites)
    tiled = spinors.reshape(sources, held, 2, spins, colours, sites // LANES, LANES)
    s_view = tiled.transpose(0, 1, 2, 4, 5, 3, 6).reshape(
        sources, held, 2, colours, SUBLANES, LANES
    )

    rows = vectors // 2
    part = rows // OUT_PIECES
    f32 = jnp.float32

    def run(m):
        vmem = pl.BlockSpec(memory_space=pltpu.VMEM)
        e_items = [(size, depth, sites) for _, size in plan]
        o_item = (part, 2 * width)
        buffers = []
        for pieces_ in (e_items, [o_item] * OUT_PIECES):
            for slots in (half, m, m, held):
                buffers += [pltpu.VMEM((slots,) + item, f32) for item in pieces_]
        return pl.pallas_call(
            functools.partial(kernel, n, m, plan),
            name=f"project_{m}",
            out_shape=jax.ShapeDtypeStruct((held, rows, 2 * width), f32),
            in_specs=[
                pl.BlockSpec(memory_space=pltpu.SMEM), vmem, pl.BlockSpec(memory_space=pl.ANY)
            ],
            out_specs=vmem,
            scratch_shapes=buffers + [
                pltpu.VMEM((held, layers, vectors, sites), f32),
                pltpu.VMEM((held, layers, 2 * width, sites), jnp.bfloat16),
                pltpu.VMEM((held, layers, 2 * width, sites), jnp.bfloat16),
                pltpu.VMEM((held, vectors, 2 * width), f32),
                pltpu.VMEM((OUT_PIECES, held) + o_item, f32),
                pltpu.VMEM((OUT_PIECES, held) + o_item, f32),
                pltpu.VMEM((OUT_PIECES, held) + o_item, f32),
                pltpu.VMEM(s_view.shape, f32),
                pltpu.SMEM((2, 2, extent), jnp.int32),
            ] + [pltpu.SemaphoreType.DMA((2, len(plan)))] * 4
            + [pltpu.SemaphoreType.DMA((2, OUT_PIECES))] * 4 + [pltpu.SemaphoreType.DMA],
            compiler_params=pltpu.CompilerParams(
                collective_id=m, has_side_effects=True, vmem_limit_bytes=48 * 1024 * 1024
            ),
        )

    branches = [run(m) for m in range(1, half + 1)]
    projected = lax.switch(jnp.maximum(count, 1) - 1, branches, group_of, e_view, s_view)
    projected = projected.reshape(held, rows, 2, sources, spins)
    first = lax.axis_index("src") * sources
    place = (source_ids[None, :] - first) == jnp.arange(sources, dtype=jnp.int32)[:, None]
    return jnp.einsum(
        "jn,rkpns->rpsjk", place.astype(f32), projected, precision=lax.Precision.HIGHEST
    )


def solution(mesh):
    in_specs = (
        P("src", "ta", None, "job", None, "xyz"),
        P("ta", "job", None, None, "xyz"),
        P(),
        P("src"),
    )
    out_specs = P("ta", None, "job", "src", "xyz")
    n = mesh.shape["ta"]
    line = n == 4 and mesh.shape["src"] == 2 and mesh.shape["xyz"] == 2

    def local(spinors, eigvecs, group_of, source_ids):
        tiles = spinors.shape[5] // LANES
        if line and tiles == 2 and tiles * spinors.shape[3] == SUBLANES:
            return local_line(n, spinors, eigvecs, group_of, source_ids)
        return local_general(spinors, eigvecs, group_of, source_ids)

    return jax.shard_map(local, mesh=mesh, in_specs=in_specs, out_specs=out_specs, check_vma=False)
```
